1024 devices in a mesh: cols: 128 (over z, y), chan: 8 (over x, core).
Axes of the slice: x: 4, y: 4, z: 32, core: 2. Of those that a mesh axis runs over, the one named last changes fastest.
Arguments:
- anomaly: bfloat16 [32768, 80, 128], P('cols'), may hold values from -6 to 6
- jacobian: bfloat16 [16384, 256, 128], P(('cols', 'chan')), may hold values from -0.5 to 0.5
- foot_cols: int32 [16384, 4], P('cols'), may hold values from 0 to 32767, as said below
- foot_weight: float32 [16384, 4], P('cols'), may hold values from 0.1 to 1
- obs_count: int32 [128], P('cols'), may hold values from 32 to 128, as said below
- obs_weight: bfloat16 [256, 16384], P(None, ('cols', 'chan')), may hold values from 0.25 to 4
Outputs:
- radiance_pert: bfloat16 [80, 256, 16384], P(None, 'chan', 'cols')
- ensemble_gram: float32 [1024, 80, 80], P('cols', 'chan')
The draws below stay inside these ranges and needn't reach their ends.
Inputs may be any that keep to these rules, and one draw needn't show every extreme that they name: `foot_cols`: the footprint columns of an observation of tile t lie among the columns t * 256 - 32 to (t + 1) * 256 + 31, taken modulo 32768. The live observations of tile t are its first obs_count[t] slots; in every draw at least one tile has all 128 slots live.
All inputs are finite; a program needn't handle non-finite values.
Results may differ from the reference program's by a relative error of at most 0.0095.
Values may be sent and summed in bfloat16 or wider, within the bound.
No kernel may reach another device: no remote copies, remote signals or barrier semaphores. Data moves between devices by JAX's collectives and lax.ppermute only.
A program may use at most 32 MiB of HBM per device.

```python
import math
from functools import partial
import jax
import jax.numpy as jnp
from jax import lax

M = 80
LEV = 128
CH = 256
TCOL = 256
OBS_DEV = 128
FP = 4
HALO = 32
PTS = 8
NCOLS = 32768
NOBS = 16384


def draw_foot_cols(key, part):
    tile_index = (jnp.arange(NOBS, dtype=jnp.int32) // OBS_DEV)[:, None]
    base_offset = jax.random.randint(jax.random.fold_in(key, 11), (NOBS, 1), -HALO, TCOL + HALO - 5, dtype=jnp.int32)
    spread_offset = jax.random.randint(jax.random.fold_in(key, 12), (NOBS, FP), 0, 6, dtype=jnp.int32)
    return jnp.mod(tile_index * TCOL + base_offset + spread_offset, NCOLS).astype(jnp.int32)


def draw_obs_count(key, part):
    tile_count = NOBS // OBS_DEV
    counts = jax.random.randint(jax.random.fold_in(key, 21), (tile_count,), OBS_DEV // 4, OBS_DEV + 1, dtype=jnp.int32)
    full_tile = jax.random.randint(jax.random.fold_in(key, 22), (), 0, tile_count, dtype=jnp.int32)
    return jnp.where(jnp.arange(tile_count, dtype=jnp.int32) == full_tile, OBS_DEV, counts).astype(jnp.int32)


def shard_levels(own_key, dims, split, least, largest):
    gain = 1.0
    for position, shards_of in split:
        steps = jax.random.uniform(jax.random.fold_in(jax.random.fold_in(own_key, 6), position), (shards_of,), jnp.float32, least / len(split), largest / len(split))
        gain = gain * jnp.repeat(jnp.exp(steps), dims[position] // shards_of).reshape((-1,) + (1,) * (len(dims) - 1 - position))
    return gain


def noise(rng, dims, deviation, most, split=(), kind=jnp.bfloat16):
    gain = shard_levels(rng, dims, split, -0.22, 0.18) if split else 1.0
    entries = jax.random.normal(rng, dims, jnp.float32) * deviation * gain
    return jnp.minimum(jnp.maximum(entries, -most), most).astype(kind)


def setup_inputs(seed: int = 0) -> dict:
    streams_of = jax.random.split(jax.random.key(seed), 7)
    return {
        "anomaly": noise(streams_of[0], (NCOLS, M, LEV), 1.0, 6.0, ((0, 128),)),
        "jacobian": noise(streams_of[1], (NOBS, CH, LEV), LEV ** -0.5, 0.5, ((0, 1024),)),
        "foot_cols": draw_foot_cols(jax.random.fold_in(streams_of[6], 71), 0),
        "foot_weight": jnp.clip(jnp.exp(math.log(1.0) - 2.3025851 * jax.random.uniform(streams_of[3], (NOBS, FP), jnp.float32) ** shard_levels(streams_of[3], (NOBS, FP), ((0, 128),), -0.2, 0.2)), 0.1, 1.0),
        "obs_count": draw_obs_count(jax.random.fold_in(streams_of[6], 71), 0),
        "obs_weight": jnp.clip(jnp.exp(math.log(4.0) - 2.7725887 * jax.random.uniform(streams_of[5], (CH, NOBS), jnp.float32) ** shard_levels(streams_of[5], (CH, NOBS), ((1, 1024),), -0.2, 0.2)), 0.25, 4.0).astype(jnp.bfloat16),
    }


def taper(distance, half_width):
    relative = jnp.abs(distance) / half_width
    near_part = ((((-0.25 * relative + 0.5) * relative + 0.625) * relative - 5.0 / 3.0) * relative * relative) + 1.0
    bounded = jnp.maximum(relative, 1.0)
    far_part = (((((relative / 12.0 - 0.5) * relative + 0.625) * relative + 5.0 / 3.0) * relative - 5.0) * relative + 4.0) - 2.0 / (3.0 * bounded)
    return jnp.where(relative <= 1.0, near_part, jnp.where(relative <= 2.0, far_part, 0.0))


def local_gram(perturbed, error_weight, centers):
    spacing = TCOL / PTS
    points = (jnp.arange(PTS, dtype=jnp.float32) + 0.5) * spacing
    locality = taper(centers[None, :] - points[:, None], spacing)
    values = perturbed.astype(jnp.float32)
    weighted = values * error_weight.astype(jnp.float32)
    flat_values = values.reshape(values.shape[0], -1)
    gram_list = []
    for point_index in range(PTS):
        scaled = (weighted * locality[point_index][None, None, :]).astype(jnp.bfloat16)
        scaled = lax.optimization_barrier(scaled)
        flat_scaled = scaled.astype(jnp.float32).reshape(values.shape[0], -1)
        gram_list.append(jnp.dot(flat_scaled, flat_values.T, preferred_element_type=jnp.float32))
    return jnp.stack(gram_list) / (CH * OBS_DEV)


def tile_work(anomaly, inputs):
    tile_index, jacobian_tile, foot_tile, foot_gain, live_count, error_weight = inputs
    mixed_cols = jnp.zeros((OBS_DEV, M, LEV), jnp.float32)
    for column_slot in range(FP):
        mixed_cols = mixed_cols + foot_gain[:, column_slot, None, None] * anomaly[foot_tile[:, column_slot]].astype(jnp.float32)
    mixed_cols = lax.optimization_barrier(mixed_cols.astype(jnp.bfloat16))
    radiance = jnp.einsum("ncl,nml->mcn", jacobian_tile.astype(jnp.float32), mixed_cols.astype(jnp.float32))
    live_mask = (jnp.arange(OBS_DEV, dtype=jnp.int32) < live_count).astype(jnp.float32)
    perturbed = (radiance * live_mask[None, None, :]).astype(jnp.bfloat16)
    offsets = jnp.mod(foot_tile - tile_index * TCOL + HALO, NCOLS) - HALO
    centers = jnp.sum(foot_gain * offsets.astype(jnp.float32), axis=1) / jnp.sum(foot_gain, axis=1)
    return perturbed, local_gram(perturbed, error_weight[None], centers)


def reference(anomaly, jacobian, foot_cols, foot_weight, obs_count, obs_weight):
    tile_count = NOBS // OBS_DEV
    per_tile = (
        jnp.arange(tile_count, dtype=jnp.int32),
        jacobian.reshape(tile_count, OBS_DEV, CH, LEV),
        foot_cols.reshape(tile_count, OBS_DEV, FP),
        foot_weight.reshape(tile_count, OBS_DEV, FP),
        obs_count,
        obs_weight.reshape(CH, tile_count, OBS_DEV).transpose(1, 0, 2),
    )
    perturbed, gram_blocks = lax.map(partial(tile_work, anomaly), per_tile)
    radiance_pert = perturbed.transpose(1, 2, 0, 3).reshape(M, CH, NOBS)
    return radiance_pert, gram_blocks.reshape(tile_count * PTS, M, M)
```

```python
import jax
import jax.numpy as jnp
from jax import lax
from jax.experimental import pallas as pl
from jax.experimental.pallas import tpu as pltpu
from jax.sharding import PartitionSpec as P


CH = 256
OBS_DEV = 128
HALO = 32
PTS = 8
FP = 4
MIB = 1024 * 1024

VMEM = pltpu.MemorySpace.VMEM
SMEM = pltpu.MemorySpace.SMEM
NT = (((1,), (1,)), ((), ()))


def taper(distance, half_width):
    relative = jnp.abs(distance) / half_width
    near_part = (
        ((-0.25 * relative + 0.5) * relative + 0.625) * relative - 5.0 / 3.0
    ) * relative * relative + 1.0
    bounded = jnp.maximum(relative, 1.0)
    far_part = (
        ((((relative / 12.0 - 0.5) * relative + 0.625) * relative + 5.0 / 3.0) * relative - 5.0)
        * relative
        + 4.0
        - 2.0 / (3.0 * bounded)
    )
    return jnp.where(relative <= 1.0, near_part, jnp.where(relative <= 2.0, far_part, 0.0))


def home_mix(ints, gains, anomaly, n, tile_cols):
    total = None
    for f in range(FP):
        col = ints[f * OBS_DEV + n] - HALO
        inside = jnp.logical_and(col >= 0, col < tile_cols)
        gain = jnp.where(inside, gains[f * OBS_DEV + n], 0.0)
        term = gain * anomaly[jnp.clip(col, 0, tile_cols - 1)].astype(jnp.float32)
        total = term if total is None else total + term
    return total


def side_mix(ints, gains, halo, n, first):
    total = None
    for f in range(FP):
        col = ints[f * OBS_DEV + n] - first
        inside = jnp.logical_and(col >= 0, col < HALO)
        gain = jnp.where(inside, gains[f * OBS_DEV + n], 0.0)
        term = gain * halo[jnp.clip(col, 0, HALO - 1)].astype(jnp.float32)
        total = term if total is None else total + term
    return total


def reaches(ints, n, tile_cols):
    cols = [ints[f * OBS_DEV + n] for f in range(FP)]
    least = jnp.minimum(jnp.minimum(cols[0], cols[1]), jnp.minimum(cols[2], cols[3]))
    most = jnp.maximum(jnp.maximum(cols[0], cols[1]), jnp.maximum(cols[2], cols[3]))
    return least < HALO, most >= HALO + tile_cols


def home_kernel(tile_cols, ints, gains, anomaly, whole, own):
    share = own.shape[0]
    first_obs = ints[FP * OBS_DEV]

    def each(n, carry):
        whole[n] = home_mix(ints, gains, anomaly, n, tile_cols).astype(whole.dtype)
        return carry

    lax.fori_loop(0, OBS_DEV, each, 0, unroll=4)

    def each_own(i, carry):
        own[i] = whole[first_obs + i]
        return carry

    lax.fori_loop(0, share, each_own, 0, unroll=4)


def add_halos(ints, gains, low, high, n, tile_cols, ref, i):
    to_low, to_high = reaches(ints, n, tile_cols)

    @pl.when(to_low)
    def _():
        ref[i] = (ref[i].astype(jnp.float32) + side_mix(ints, gains, low, n, 0)).astype(ref.dtype)

    @pl.when(to_high)
    def _():
        ref[i] = (
            ref[i].astype(jnp.float32) + side_mix(ints, gains, high, n, HALO + tile_cols)
        ).astype(ref.dtype)


def gram_kernel(tile_cols, ints, gains, low, high, own, jac, weight, gram, mixed, products, turned):
    share = own.shape[0]
    members = own.shape[1]
    first_obs = ints[FP * OBS_DEV]
    live_count = ints[FP * OBS_DEV + 1]
    mixed[...] = own[...]

    def each(i, carry):
        add_halos(ints, gains, low, high, first_obs + i, tile_cols, mixed, i)
        return carry

    lax.fori_loop(0, share, each, 0)
    for i in range(share):
        live = jnp.where(first_obs + i < live_count, 1.0, 0.0)
        radiance = lax.dot_general(mixed[i], jac[i], NT, preferred_element_type=jnp.float32)
        pert = (radiance * live).astype(jnp.bfloat16)
        scaled = (pert.astype(jnp.float32) * weight[i : i + 1, :].astype(jnp.float32)).astype(
            jnp.bfloat16
        )
        products[i] = lax.dot_general(scaled, pert, NT, preferred_element_type=jnp.float32)
    for p in range(PTS):
        total = None
        for i in range(share):
            term = gains[FP * OBS_DEV + p * share + i] * products[i]
            total = term if total is None else total + term
        turned[pl.ds(p, members, stride=PTS), 0:members] = total
    gram[...] = turned[:, 0:members].reshape(members, PTS, members).astype(gram.dtype)


def mix_kernel(tile_cols, ints, gains, low, high, home, after, mixed):
    def each(n, carry):
        mixed[n] = home[n]
        add_halos(ints, gains, low, high, n, tile_cols, mixed, n)
        return carry

    lax.fori_loop(0, OBS_DEV, each, 0)


def params(mib):
    return pltpu.CompilerParams(vmem_limit_bytes=mib * MIB)


def cost(flops, bytes_accessed):
    return pl.CostEstimate(flops=flops, bytes_accessed=bytes_accessed, transcendentals=0)


def specs(*spaces):
    return [pl.BlockSpec(memory_space=space) for space in spaces]


def shards(anomaly, jacobian, foot_cols, foot_weight, obs_count, obs_weight):
    col_groups = lax.axis_size("cols")
    chans = lax.axis_size("chan")
    tile_index = lax.axis_index("cols")
    chan_index = lax.axis_index("chan")
    tile_cols, members, levels = anomaly.shape
    obs_share = jacobian.shape[0]
    block = CH // chans

    forward = [(i, (i + 1) % col_groups) for i in range(col_groups)]
    backward = [(target, source) for source, target in forward]
    low = lax.ppermute(anomaly[tile_cols - HALO :], "cols", forward)
    high = lax.ppermute(anomaly[:HALO], "cols", backward)

    pieces = jacobian.reshape(obs_share, chans, block, levels).transpose(1, 0, 2, 3)
    jac_block = lax.all_to_all(pieces, "chan", split_axis=0, concat_axis=0, tiled=True)
    jac_block = jac_block.reshape(OBS_DEV, block, levels)

    first_obs = chan_index * obs_share
    columns = foot_cols.T
    column_gains = foot_weight.T
    offsets = jnp.mod(columns - tile_index * tile_cols + HALO, tile_cols * col_groups)
    centers = jnp.sum(column_gains * (offsets - HALO).astype(jnp.float32), axis=0) / jnp.sum(
        column_gains, axis=0
    )
    own_centers = lax.dynamic_slice_in_dim(centers, first_obs, obs_share, 0)
    spacing = tile_cols / PTS
    points = (jnp.arange(PTS, dtype=jnp.float32) + 0.5) * spacing
    locality = taper(own_centers[None, :] - points[:, None], spacing) / (CH * OBS_DEV)
    ints = jnp.concatenate(
        [offsets.reshape(-1), first_obs[None].astype(jnp.int32), obs_count.astype(jnp.int32)]
    )
    gains = jnp.concatenate([column_gains.reshape(-1), locality.reshape(-1)])

    tile = jax.ShapeDtypeStruct((OBS_DEV, members, levels), jnp.bfloat16)
    share = jax.ShapeDtypeStruct((obs_share, members, levels), jnp.bfloat16)
    home, own = pl.pallas_call(
        lambda *refs: home_kernel(tile_cols, *refs),
        out_shape=(tile, share),
        in_specs=specs(SMEM, SMEM, VMEM),
        out_specs=tuple(specs(VMEM, VMEM)),
        compiler_params=params(24),
        cost_estimate=cost(4_000_000_000, 8_000_000),
        name="home_mix",
    )(ints, gains, anomaly)

    gram = pl.pallas_call(
        lambda *refs: gram_kernel(tile_cols, *refs),
        out_shape=jax.ShapeDtypeStruct((members, PTS, members), jnp.bfloat16),
        in_specs=specs(SMEM, SMEM, VMEM, VMEM, VMEM, VMEM, VMEM),
        out_specs=pl.BlockSpec(memory_space=VMEM),
        scratch_shapes=[
            pltpu.VMEM((obs_share, members, levels), jnp.bfloat16),
            pltpu.VMEM((obs_share, members, members), jnp.float32),
            pltpu.VMEM((members * PTS, 128), jnp.float32),
        ],
        compiler_params=params(16),
        cost_estimate=cost(2_000_000_000, 3_000_000),
        name="gram",
    )(ints, gains, low, high, own, jacobian, obs_weight.T)
    arrived = lax.all_to_all(gram, "chan", split_axis=0, concat_axis=0, tiled=True)

    mixed = pl.pallas_call(
        lambda *refs: mix_kernel(tile_cols, *refs),
        out_shape=tile,
        in_specs=specs(SMEM, SMEM, VMEM, VMEM, VMEM, pl.ANY),
        out_specs=pl.BlockSpec(memory_space=VMEM),
        compiler_params=params(16),
        cost_estimate=cost(2_000_000_000, 6_000_000),
        name="tile_mix",
    )(ints, gains, low, high, home, gram)
    radiance = jnp.einsum("ncl,nml->mcn", jac_block, mixed, preferred_element_type=jnp.float32)
    live_mask = (jnp.arange(OBS_DEV, dtype=jnp.int32) < obs_count[0]).astype(jnp.float32)
    perturbed = (radiance * live_mask[None, None, :]).astype(jnp.bfloat16)

    gram_rows = arrived.reshape(chans, members // chans, PTS, members).astype(jnp.float32).sum(0)
    return perturbed, gram_rows.transpose(1, 0, 2)


def solution(mesh):
    return jax.shard_map(
        shards,
        mesh=mesh,
        in_specs=(
            P("cols", None, None),
            P(("cols", "chan"), None, None),
            P("cols", None),
            P("cols", None),
            P("cols"),
            P(None, ("cols", "chan")),
        ),
        out_specs=(P(None, "chan", "cols"), P("cols", "chan", None)),
        check_vma=False,
    )
```

```python
import jax
import jax.numpy as jnp
from jax import lax
from jax.experimental import pallas as pl
from jax.experimental.pallas import tpu as pltpu
from jax.sharding import PartitionSpec as P


CH = 256
OBS_DEV = 128
HALO = 32
PTS = 8
FP = 4
MIB = 1024 * 1024

VMEM = pltpu.MemorySpace.VMEM
SMEM = pltpu.MemorySpace.SMEM
NT = (((1,), (1,)), ((), ()))


def taper(distance, half_width):
    relative = jnp.abs(distance) / half_width
    near_part = (
        ((-0.25 * relative + 0.5) * relative + 0.625) * relative - 5.0 / 3.0
    ) * relative * relative + 1.0
    bounded = jnp.maximum(relative, 1.0)
    far_part = (
        ((((relative / 12.0 - 0.5) * relative + 0.625) * relative + 5.0 / 3.0) * relative - 5.0)
        * relative
        + 4.0
        - 2.0 / (3.0 * bounded)
    )
    return jnp.where(relative <= 1.0, near_part, jnp.where(relative <= 2.0, far_part, 0.0))


def home_mix(ints, gains, anomaly, n, tile_cols):
    total = None
    for f in range(FP):
        col = ints[f * OBS_DEV + n] - HALO
        inside = jnp.logical_and(col >= 0, col < tile_cols)
        gain = jnp.where(inside, gains[f * OBS_DEV + n], 0.0)
        term = gain * anomaly[jnp.clip(col, 0, tile_cols - 1)].astype(jnp.float32)
        total = term if total is None else total + term
    return total


def side_mix(ints, gains, halo, n, first):
    total = None
    for f in range(FP):
        col = ints[f * OBS_DEV + n] - first
        inside = jnp.logical_and(col >= 0, col < HALO)
        gain = jnp.where(inside, gains[f * OBS_DEV + n], 0.0)
        term = gain * halo[jnp.clip(col, 0, HALO - 1)].astype(jnp.float32)
        total = term if total is None else total + term
    return total


def edge_kernel(anomaly, edge, sem):
    core = lax.rem(lax.axis_index("chan"), 2)
    first = jnp.where(core == 0, anomaly.shape[0] - HALO, 0)
    copy = pltpu.make_async_copy(anomaly.at[pl.ds(first, HALO)], edge, sem)
    copy.start()
    copy.wait()


def home_kernel(tile_cols, ints, gains, anomaly, home):
    def each(n, carry):
        home[n] = home_mix(ints, gains, anomaly, n, tile_cols).astype(home.dtype)
        return carry

    lax.fori_loop(0, OBS_DEV, each, 0, unroll=4)


def gram_kernel(tile_cols, ints, gains, ours, theirs, home, jac, weight, gram, mixed, perts, products, turned):
    share, members = perts.shape[:2]
    tail = (FP + 1) * OBS_DEV
    first_obs = ints[tail]
    live_count = ints[tail + 1]
    first_ours = ints[tail + 2]
    first_theirs = HALO + tile_cols - first_ours
    mixed[...] = home[...]

    def add(n, halo, first):
        mixed[n] = (mixed[n].astype(jnp.float32) + side_mix(ints, gains, halo, n, first)).astype(
            mixed.dtype
        )

    def each(n, carry):
        reach = ints[FP * OBS_DEV + n]

        @pl.when(reach > 0)
        def _():
            @pl.when(jnp.bitwise_and(reach, 1) > 0)
            def _():
                add(n, ours, first_ours)

            @pl.when(jnp.bitwise_and(reach, 2) > 0)
            def _():
                add(n, theirs, first_theirs)

        return carry

    lax.fori_loop(0, OBS_DEV, each, 0, unroll=4)
    for i in range(share):
        live = jnp.where(first_obs + i < live_count, 1.0, 0.0)
        radiance = lax.dot_general(
            mixed[first_obs + i], jac[i], NT, preferred_element_type=jnp.float32
        )
        perts[i] = (radiance * live).astype(jnp.bfloat16)
    for i in range(share):
        pert = perts[i]
        scaled = (pert.astype(jnp.float32) * weight[i : i + 1, :].astype(jnp.float32)).astype(
            jnp.bfloat16
        )
        products[i] = lax.dot_general(scaled, pert, NT, preferred_element_type=jnp.float32)
    for p in range(PTS):
        total = None
        for i in range(share):
            term = gains[FP * OBS_DEV + p * share + i] * products[i]
            total = term if total is None else total + term
        turned[pl.ds(p, members, stride=PTS), 0:members] = total
    gram[...] = turned[:, 0:members].reshape(members, PTS, members).astype(gram.dtype)


def params(mib):
    return pltpu.CompilerParams(vmem_limit_bytes=mib * MIB)


def cost(flops, bytes_accessed):
    return pl.CostEstimate(flops=flops, bytes_accessed=bytes_accessed, transcendentals=0)


def specs(*spaces):
    return [pl.BlockSpec(memory_space=space) for space in spaces]


def shards(anomaly, jacobian, foot_cols, foot_weight, obs_count, obs_weight):
    col_groups = lax.axis_size("cols")
    chans = lax.axis_size("chan")
    tile_index = lax.axis_index("cols")
    chan_index = lax.axis_index("chan")
    tile_cols, members, levels = anomaly.shape
    obs_share = jacobian.shape[0]
    block = CH // chans

    core = lax.rem(chan_index, 2)
    edge = pl.pallas_call(
        edge_kernel,
        out_shape=jax.ShapeDtypeStruct((HALO, members, levels), jnp.bfloat16),
        in_specs=specs(pl.ANY),
        out_specs=pl.BlockSpec(memory_space=VMEM),
        scratch_shapes=[pltpu.SemaphoreType.DMA],
        compiler_params=params(59),
        cost_estimate=cost(1_000_000, 1_300_000),
        name="edge",
    )(anomaly)
    to_side = [
        (t * chans + j, (t + (1 if j % 2 == 0 else -1)) % col_groups * chans + j)
        for t in range(col_groups)
        for j in range(chans)
    ]
    ours = lax.ppermute(edge, ("cols", "chan"), to_side)
    theirs = lax.ppermute(ours, "chan", [(j, j ^ 1) for j in range(chans)])

    pieces = jacobian.reshape(obs_share, chans, block, levels).transpose(1, 0, 2, 3)
    jac_block = lax.all_to_all(pieces, "chan", split_axis=0, concat_axis=0, tiled=True)
    jac_block = jac_block.reshape(OBS_DEV, block, levels)

    first_obs = chan_index * obs_share
    columns = foot_cols.T
    column_gains = foot_weight.T
    offsets = jnp.mod(columns - tile_index * tile_cols + HALO, tile_cols * col_groups)
    centers = jnp.sum(column_gains * (offsets - HALO).astype(jnp.float32), axis=0) / jnp.sum(
        column_gains, axis=0
    )
    own_centers = lax.dynamic_slice_in_dim(centers, first_obs, obs_share, 0)
    spacing = tile_cols / PTS
    points = (jnp.arange(PTS, dtype=jnp.float32) + 0.5) * spacing
    locality = taper(own_centers[None, :] - points[:, None], spacing) / (CH * OBS_DEV)
    first_ours = jnp.where(core == 0, 0, HALO + tile_cols)
    low_reach = jnp.min(offsets, axis=0) < HALO
    high_reach = jnp.max(offsets, axis=0) >= HALO + tile_cols
    ours_reach = jnp.where(core == 0, low_reach, high_reach)
    theirs_reach = jnp.where(core == 0, high_reach, low_reach)
    reach = ours_reach.astype(jnp.int32) + 2 * theirs_reach.astype(jnp.int32)
    tail = jnp.stack([first_obs, obs_count[0], first_ours]).astype(jnp.int32)
    ints = jnp.concatenate([offsets.reshape(-1), reach, tail])
    gains = jnp.concatenate([column_gains.reshape(-1), locality.reshape(-1)])

    tile = jax.ShapeDtypeStruct((OBS_DEV, members, levels), jnp.bfloat16)
    home = pl.pallas_call(
        lambda *refs: home_kernel(tile_cols, *refs),
        out_shape=tile,
        in_specs=specs(SMEM, SMEM, VMEM),
        out_specs=pl.BlockSpec(memory_space=VMEM),
        compiler_params=params(12),
        cost_estimate=cost(4_000_000_000, 8_000_000),
        name="home_mix",
    )(ints, gains, anomaly)

    gram, mixed = pl.pallas_call(
        lambda *refs: gram_kernel(tile_cols, *refs),
        out_shape=(jax.ShapeDtypeStruct((members, PTS, members), jnp.bfloat16), tile),
        in_specs=specs(SMEM, SMEM, VMEM, VMEM, VMEM, VMEM, VMEM),
        out_specs=tuple(specs(VMEM, VMEM)),
        scratch_shapes=[
            pltpu.VMEM((obs_share, members, CH), jnp.bfloat16),
            pltpu.VMEM((obs_share, members, members), jnp.float32),
            pltpu.VMEM((members * PTS, 128), jnp.float32),
        ],
        compiler_params=params(16),
        cost_estimate=cost(6_000_000_000, 3_000_000),
        name="gram",
    )(ints, gains, ours, theirs, home, jacobian, obs_weight.T)
    arrived = lax.all_to_all(gram, "chan", split_axis=0, concat_axis=0, tiled=True)
    radiance = jnp.einsum("ncl,nml->mcn", jac_block, mixed, preferred_element_type=jnp.float32)
    live_mask = (jnp.arange(OBS_DEV, dtype=jnp.int32) < obs_count[0]).astype(jnp.float32)
    perturbed = (radiance * live_mask[None, None, :]).astype(jnp.bfloat16)

    gram_rows = arrived.reshape(chans, members // chans, PTS, members).astype(jnp.float32).sum(0)
    return perturbed, gram_rows.transpose(1, 0, 2)


def solution(mesh):
    return jax.shard_map(
        shards,
        mesh=mesh,
        in_specs=(
            P("cols", None, None),
            P(("cols", "chan"), None, None),
            P("cols", None),
            P("cols", None),
            P("cols"),
            P(None, ("cols", "chan")),
        ),
        out_specs=(P(None, "chan", "cols"), P("cols", "chan", None)),
        check_vma=False,
    )
```

```python
import jax
import jax.numpy as jnp
from jax import lax
from jax.experimental import pallas as pl
from jax.experimental.pallas import tpu as pltpu
from jax.sharding import PartitionSpec as P


CH = 256
OBS_DEV = 128
HALO = 32
PTS = 8
FP = 4
MIB = 1024 * 1024
REACH = FP * OBS_DEV
TAIL = REACH + OBS_DEV
HOME_COLS = TAIL + 2
LOCALITY = FP * OBS_DEV
HOME_GAINS = LOCALITY + OBS_DEV

VMEM = pltpu.MemorySpace.VMEM
SMEM = pltpu.MemorySpace.SMEM
NT = (((1,), (1,)), ((), ()))


def taper(distance, half_width):
    relative = jnp.abs(distance) / half_width
    near_part = (
        ((-0.25 * relative + 0.5) * relative + 0.625) * relative - 5.0 / 3.0
    ) * relative * relative + 1.0
    bounded = jnp.maximum(relative, 1.0)
    far_part = (
        ((((relative / 12.0 - 0.5) * relative + 0.625) * relative + 5.0 / 3.0) * relative - 5.0)
        * relative
        + 4.0
        - 2.0 / (3.0 * bounded)
    )
    return jnp.where(relative <= 1.0, near_part, jnp.where(relative <= 2.0, far_part, 0.0))


def side_mix(ints, gains, halo, n, first):
    total = None
    for f in range(FP):
        col = ints[f * OBS_DEV + n] - first
        inside = jnp.logical_and(col >= 0, col < HALO)
        gain = jnp.where(inside, gains[f * OBS_DEV + n], 0.0)
        term = gain * halo[jnp.clip(col, 0, HALO - 1)].astype(jnp.float32)
        total = term if total is None else total + term
    return total


def home_kernel(ints, gains, anomaly, home, tile, sems):
    members = anomaly.shape[1]
    cuts = (0, 48, members)
    parts = [pl.ds(low, high - low) for low, high in zip(cuts, cuts[1:])]
    copies = [
        pltpu.make_async_copy(anomaly.at[:, part], tile.at[:, part], sems.at[k])
        for k, part in enumerate(parts)
    ]
    for copy in copies:
        copy.start()
    for copy, part in zip(copies, parts):
        copy.wait()

        def each(n, carry, part=part):
            total = None
            for f in range(FP):
                gain = gains[HOME_GAINS + f * OBS_DEV + n]
                term = gain * tile[ints[HOME_COLS + f * OBS_DEV + n], part].astype(jnp.float32)
                total = term if total is None else total + term
            home[n, part] = total.astype(home.dtype)
            return carry

        lax.fori_loop(0, OBS_DEV, each, 0, unroll=4)


def gram_kernel(tile_cols, count, ints, gains, ours, theirs, home, jac, weight, gram, mixed, perts, products, turned):
    share, members = perts.shape[:2]
    first_obs = ints[TAIL]
    live_count = count[0]
    first_ours = ints[TAIL + 1]
    first_theirs = HALO + tile_cols - first_ours

    def add(n, halo, first):
        mixed[n] = (mixed[n].astype(jnp.float32) + side_mix(ints, gains, halo, n, first)).astype(
            mixed.dtype
        )

    def complete(n):
        reach = ints[REACH + n]

        @pl.when(reach > 0)
        def _():
            @pl.when(jnp.bitwise_and(reach, 1) > 0)
            def _():
                add(n, ours, first_ours)

            @pl.when(jnp.bitwise_and(reach, 2) > 0)
            def _():
                add(n, theirs, first_theirs)

    def each(q, carry):
        batch = pl.ds(q * 4, 4)
        mixed[batch] = home[batch]
        for k in range(4):
            complete(q * 4 + k)
        return carry

    lax.fori_loop(0, OBS_DEV // 4, each, 0)
    for i in range(share):
        live = jnp.where(first_obs + i < live_count, 1.0, 0.0)
        radiance = lax.dot_general(
            mixed[first_obs + i], jac[i], NT, preferred_element_type=jnp.float32
        )
        perts[i] = (radiance * live).astype(jnp.bfloat16)
    for i in range(share):
        pert = perts[i]
        scaled = (pert.astype(jnp.float32) * weight[i : i + 1, :].astype(jnp.float32)).astype(
            jnp.bfloat16
        )
        products[i] = lax.dot_general(scaled, pert, NT, preferred_element_type=jnp.float32)
    for p in range(PTS):
        total = None
        for i in range(share):
            term = gains[LOCALITY + p * share + i] * products[i]
            total = term if total is None else total + term
        turned[pl.ds(p, members, stride=PTS), 0:members] = total
    gram[...] = turned[:, 0:members].reshape(members, PTS, members).astype(gram.dtype)


def radiance_kernel(count, jac, mixed_ref, out, mixed, turned, sems):
    members, block, levels = mixed.shape[1], jac.shape[1], jac.shape[2]
    steps = sems.shape[0]
    packs = levels // block
    groups = OBS_DEV // packs
    pitch = groups + 8
    owner = lax.broadcasted_iota(jnp.int32, (members, levels), 1) // block

    batch = groups // steps
    copies = [
        [
            pltpu.make_async_copy(
                mixed_ref.at[pl.ds(j * groups + step * batch, batch)],
                mixed.at[pl.ds(j * groups + step * batch, batch)],
                sems.at[step, j],
            )
            for j in range(packs)
        ]
        for step in range(steps)
    ]
    for step in copies:
        for copy in step:
            copy.start()

    def group(g, carry):
        names = [g + j * groups for j in range(packs)]
        stacked = jnp.concatenate([jac[n] for n in names], axis=0)
        kept = None
        for j, n in enumerate(names):
            part = lax.dot_general(mixed[n], stacked, NT, preferred_element_type=jnp.float32)
            kept = part if kept is None else jnp.where(owner == j, part, kept)
        turned[pl.ds(g, members, stride=pitch), :] = kept
        return carry

    for step in range(steps):
        for copy in copies[step]:
            copy.wait()
        lax.fori_loop(step * batch, (step + 1) * batch, group, 0, unroll=4)
    slot = lax.broadcasted_iota(jnp.int32, (block, OBS_DEV), 1)
    spot = slot // groups
    live = slot < count[0]

    def members_of(q, carry):
        rows = [
            turned[pl.ds(pl.multiple_of((q * packs + k) * pitch, 8), groups), :]
            for k in range(packs)
        ]
        flipped = jnp.concatenate(rows, axis=0).T
        for k in range(packs):
            kept = None
            for j in range(packs):
                piece = flipped[j * block : (j + 1) * block, :]
                shift = (j - k) * groups % OBS_DEV
                piece = piece if shift == 0 else pltpu.roll(piece, shift, 1)
                kept = piece if kept is None else jnp.where(spot == j, piece, kept)
            out[q * packs + k] = jnp.where(live, kept, 0.0).astype(out.dtype)
        return carry

    lax.fori_loop(0, members // packs, members_of, 0, unroll=2)


def params(mib):
    return pltpu.CompilerParams(vmem_limit_bytes=mib * MIB)


def cost(flops, bytes_accessed):
    return pl.CostEstimate(flops=flops, bytes_accessed=bytes_accessed, transcendentals=0)


def specs(*spaces):
    return [pl.BlockSpec(memory_space=space) for space in spaces]


def shards(anomaly, jacobian, foot_cols, foot_weight, obs_count, obs_weight):
    col_groups = lax.axis_size("cols")
    chans = lax.axis_size("chan")
    tile_index = lax.axis_index("cols")
    chan_index = lax.axis_index("chan")
    tile_cols, members, levels = anomaly.shape
    obs_share = jacobian.shape[0]
    block = CH // chans

    core = lax.rem(chan_index, 2)
    edge = lax.dynamic_slice_in_dim(
        anomaly, jnp.where(core == 0, tile_cols - HALO, 0), HALO, 0
    )
    to_side = [
        (t * chans + j, (t + (1 if j % 2 == 0 else -1)) % col_groups * chans + j)
        for t in range(col_groups)
        for j in range(chans)
    ]
    ours = lax.ppermute(edge, ("cols", "chan"), to_side)
    theirs = lax.ppermute(ours, "chan", [(j, j ^ 1) for j in range(chans)])

    pieces = jacobian.reshape(obs_share, chans, block, levels).transpose(1, 0, 2, 3)
    jac_block = lax.all_to_all(pieces, "chan", split_axis=0, concat_axis=0, tiled=True)
    jac_block = jac_block.reshape(OBS_DEV, block, levels)

    first_obs = chan_index * obs_share
    columns = foot_cols.T
    column_gains = foot_weight.T
    offsets = jnp.mod(columns - tile_index * tile_cols + HALO, tile_cols * col_groups)
    centers = jnp.sum(column_gains * (offsets - HALO).astype(jnp.float32), axis=0) / jnp.sum(
        column_gains, axis=0
    )
    own_centers = lax.dynamic_slice_in_dim(centers, first_obs, obs_share, 0)
    spacing = tile_cols / PTS
    points = (jnp.arange(PTS, dtype=jnp.float32) + 0.5) * spacing
    locality = taper(own_centers[None, :] - points[:, None], spacing) / (CH * OBS_DEV)
    first_ours = jnp.where(core == 0, 0, HALO + tile_cols)
    low_reach = jnp.min(offsets, axis=0) < HALO
    high_reach = jnp.max(offsets, axis=0) >= HALO + tile_cols
    ours_reach = jnp.where(core == 0, low_reach, high_reach)
    theirs_reach = jnp.where(core == 0, high_reach, low_reach)
    reach = ours_reach.astype(jnp.int32) + 2 * theirs_reach.astype(jnp.int32)
    tail = jnp.stack([first_obs, first_ours]).astype(jnp.int32)
    inside = jnp.logical_and(offsets >= HALO, offsets < HALO + tile_cols)
    home_cols = jnp.clip(offsets - HALO, 0, tile_cols - 1)
    home_gains = jnp.where(inside, column_gains, 0.0)
    ints = jnp.concatenate([offsets.reshape(-1), reach, tail, home_cols.reshape(-1)])
    gains = jnp.concatenate(
        [column_gains.reshape(-1), locality.reshape(-1), home_gains.reshape(-1)]
    )

    tile = jax.ShapeDtypeStruct((OBS_DEV, members, levels), jnp.bfloat16)
    home = pl.pallas_call(
        home_kernel,
        out_shape=tile,
        in_specs=specs(SMEM, SMEM, pl.ANY),
        out_specs=pl.BlockSpec(memory_space=VMEM),
        scratch_shapes=[pltpu.VMEM(anomaly.shape, anomaly.dtype), pltpu.SemaphoreType.DMA((2,))],
        compiler_params=params(50),
        cost_estimate=cost(4_000_000_000, 8_000_000),
        name="home_mix",
    )(ints, gains, anomaly)

    gram, mixed = pl.pallas_call(
        lambda *refs: gram_kernel(tile_cols, *refs),
        out_shape=(jax.ShapeDtypeStruct((members, PTS, members), jnp.bfloat16), tile),
        in_specs=specs(SMEM, SMEM, SMEM, VMEM, VMEM, VMEM, VMEM, VMEM),
        out_specs=tuple(specs(VMEM, VMEM)),
        scratch_shapes=[
            pltpu.VMEM((obs_share, members, CH), jnp.bfloat16),
            pltpu.VMEM((obs_share, members, members), jnp.float32),
            pltpu.VMEM((members * PTS, 128), jnp.float32),
        ],
        compiler_params=params(16),
        cost_estimate=cost(6_000_000_000, 3_000_000),
        name="gram",
    )(obs_count, ints, gains, ours, theirs, home, jacobian, obs_weight.T)
    arrived = lax.all_to_all(gram, "chan", split_axis=0, concat_axis=0, tiled=True)
    perturbed = pl.pallas_call(
        radiance_kernel,
        out_shape=jax.ShapeDtypeStruct((members, block, OBS_DEV), jnp.bfloat16),
        in_specs=specs(SMEM, VMEM, pl.ANY),
        out_specs=pl.BlockSpec(memory_space=VMEM),
        scratch_shapes=[
            pltpu.VMEM(tile.shape, tile.dtype),
            pltpu.VMEM((members * (OBS_DEV * block // levels + 8), levels), jnp.float32),
            pltpu.SemaphoreType.DMA((4, levels // block)),
        ],
        compiler_params=params(52),
        cost_estimate=cost(4_000_000_000, 5_000_000),
        name="radiance",
    )(obs_count, jac_block, mixed)

    gram_rows = arrived.reshape(chans, members // chans, PTS, members).astype(jnp.float32).sum(0)
    return perturbed, gram_rows.transpose(1, 0, 2)


def solution(mesh):
    return jax.shard_map(
        shards,
        mesh=mesh,
        in_specs=(
            P("cols", None, None),
            P(("cols", "chan"), None, None),
            P("cols", None),
            P("cols", None),
            P("cols"),
            P(None, ("cols", "chan")),
        ),
        out_specs=(P(None, "chan", "cols"), P("cols", "chan", None)),
        check_vma=False,
    )
```

```python
import jax
import jax.numpy as jnp
from jax import lax
from jax.experimental import pallas as pl
from jax.experimental.pallas import tpu as pltpu
from jax.sharding import PartitionSpec as P


CH = 256
OBS_DEV = 128
HALO = 32
PTS = 8
FP = 4
MIB = 1024 * 1024
REACH = FP * OBS_DEV
TAIL = REACH + OBS_DEV
HOME_COLS = TAIL + 2
LOCALITY = FP * OBS_DEV
HOME_GAINS = LOCALITY + OBS_DEV

VMEM = pltpu.MemorySpace.VMEM
SMEM = pltpu.MemorySpace.SMEM
NT = (((1,), (1,)), ((), ()))


def taper(distance, half_width):
    relative = jnp.abs(distance) / half_width
    near_part = (
        ((-0.25 * relative + 0.5) * relative + 0.625) * relative - 5.0 / 3.0
    ) * relative * relative + 1.0
    bounded = jnp.maximum(relative, 1.0)
    far_part = (
        ((((relative / 12.0 - 0.5) * relative + 0.625) * relative + 5.0 / 3.0) * relative - 5.0)
        * relative
        + 4.0
        - 2.0 / (3.0 * bounded)
    )
    return jnp.where(relative <= 1.0, near_part, jnp.where(relative <= 2.0, far_part, 0.0))


def side_mix(ints, gains, halo, n, first):
    total = None
    for f in range(FP):
        col = ints[f * OBS_DEV + n] - first
        inside = jnp.logical_and(col >= 0, col < HALO)
        gain = jnp.where(inside, gains[f * OBS_DEV + n], 0.0)
        term = gain * halo[jnp.clip(col, 0, HALO - 1)].astype(jnp.float32)
        total = term if total is None else total + term
    return total


def prepare_kernel(anomaly, jac, edge, pieces, cut, held, cut_sems, in_sems, out_sems):
    core = lax.rem(lax.axis_index("chan"), 2)
    first = jnp.where(core == 0, anomaly.shape[0] - HALO, 0)
    chans, _, block, _ = held.shape
    cut_in = pltpu.make_async_copy(anomaly.at[pl.ds(first, HALO)], cut, cut_sems.at[0])
    cut_out = pltpu.make_async_copy(cut, edge, cut_sems.at[1])
    cut_in.start()
    arrive = [
        pltpu.make_async_copy(jac.at[:, pl.ds(j * block, block)], held.at[j], in_sems.at[j])
        for j in range(chans)
    ]
    leave = [
        pltpu.make_async_copy(held.at[j], pieces.at[j], out_sems.at[j]) for j in range(chans)
    ]
    for copy in arrive:
        copy.start()
    cut_in.wait()
    cut_out.start()
    for before, after in zip(arrive, leave):
        before.wait()
        after.start()
    cut_out.wait()
    for copy in leave:
        copy.wait()


def home_kernel(ints, gains, anomaly, home, tile, sems):
    members = anomaly.shape[1]
    cuts = (0, 48, members)
    parts = [pl.ds(low, high - low) for low, high in zip(cuts, cuts[1:])]
    copies = [
        pltpu.make_async_copy(anomaly.at[:, part], tile.at[:, part], sems.at[k])
        for k, part in enumerate(parts)
    ]
    for copy in copies:
        copy.start()
    for copy, part in zip(copies, parts):
        copy.wait()

        def each(n, carry, part=part):
            total = None
            for f in range(FP):
                gain = gains[HOME_GAINS + f * OBS_DEV + n]
                term = gain * tile[ints[HOME_COLS + f * OBS_DEV + n], part].astype(jnp.float32)
                total = term if total is None else total + term
            home[n, part] = total.astype(home.dtype)
            return carry

        lax.fori_loop(0, OBS_DEV, each, 0, unroll=4)


def gram_kernel(tile_cols, count, ints, gains, ours, theirs, home, jac, weight, gram, mixed_out, mixed, perts, products, turned, sem):
    share, members = perts.shape[:2]
    first_obs = ints[TAIL]
    live_count = count[0]
    first_ours = ints[TAIL + 1]
    first_theirs = HALO + tile_cols - first_ours

    def add(n, halo, first):
        mixed[n] = (mixed[n].astype(jnp.float32) + side_mix(ints, gains, halo, n, first)).astype(
            mixed.dtype
        )

    def complete(n):
        reach = ints[REACH + n]

        @pl.when(reach > 0)
        def _():
            @pl.when(jnp.bitwise_and(reach, 1) > 0)
            def _():
                add(n, ours, first_ours)

            @pl.when(jnp.bitwise_and(reach, 2) > 0)
            def _():
                add(n, theirs, first_theirs)

    def each(q, carry):
        batch = pl.ds(q * 4, 4)
        mixed[batch] = home[batch]
        for k in range(4):
            complete(q * 4 + k)
        return carry

    lax.fori_loop(0, OBS_DEV // 4, each, 0)
    leave = pltpu.make_async_copy(mixed, mixed_out, sem)
    leave.start()
    for i in range(share):
        live = jnp.where(first_obs + i < live_count, 1.0, 0.0)
        radiance = lax.dot_general(
            mixed[first_obs + i], jac[i], NT, preferred_element_type=jnp.float32
        )
        perts[i] = (radiance * live).astype(jnp.bfloat16)
    for i in range(share):
        pert = perts[i]
        scaled = (pert.astype(jnp.float32) * weight[i : i + 1, :].astype(jnp.float32)).astype(
            jnp.bfloat16
        )
        products[i] = lax.dot_general(scaled, pert, NT, preferred_element_type=jnp.float32)
    for p in range(PTS):
        total = None
        for i in range(share):
            term = gains[LOCALITY + p * share + i] * products[i]
            total = term if total is None else total + term
        turned[pl.ds(p, members, stride=PTS), 0:members] = total
    gram[...] = turned[:, 0:members].reshape(members, PTS, members).astype(gram.dtype)
    leave.wait()


def radiance_kernel(count, jac, mixed_ref, out, mixed, turned, sems):
    members, block, levels = mixed.shape[1], jac.shape[1], jac.shape[2]
    steps = sems.shape[0]
    packs = levels // block
    groups = OBS_DEV // packs
    pitch = groups + 8
    owner = lax.broadcasted_iota(jnp.int32, (members, levels), 1) // block

    batch = groups // steps
    copies = [
        [
            pltpu.make_async_copy(
                mixed_ref.at[pl.ds(j * groups + step * batch, batch)],
                mixed.at[pl.ds(j * groups + step * batch, batch)],
                sems.at[step, j],
            )
            for j in range(packs)
        ]
        for step in range(steps)
    ]
    for step in copies:
        for copy in step:
            copy.start()

    def group(g, carry):
        names = [g + j * groups for j in range(packs)]
        stacked = jnp.concatenate([jac[n] for n in names], axis=0)
        averages = jnp.concatenate([mixed[n] for n in names], axis=0)
        full = lax.dot_general(averages, stacked, NT, preferred_element_type=jnp.float32)
        kept = full[:members]
        for j in range(1, packs):
            kept = jnp.where(owner == j, full[j * members : (j + 1) * members], kept)
        turned[pl.ds(g, members, stride=pitch), :] = kept
        return carry

    for step in range(steps):
        for copy in copies[step]:
            copy.wait()
        lax.fori_loop(step * batch, (step + 1) * batch, group, 0, unroll=batch)
    slot = lax.broadcasted_iota(jnp.int32, (block, OBS_DEV), 1)
    spot = slot // groups
    live = slot < count[0]

    def members_of(q, carry):
        rows = [
            turned[pl.ds(pl.multiple_of((q * packs + k) * pitch, 8), groups), :].astype(out.dtype)
            for k in range(packs)
        ]
        flipped = jnp.concatenate(rows, axis=0).T
        for k in range(packs):
            kept = None
            for j in range(packs):
                piece = flipped[j * block : (j + 1) * block, :]
                shift = (j - k) * groups % OBS_DEV
                piece = piece if shift == 0 else pltpu.roll(piece, shift, 1)
                kept = piece if kept is None else jnp.where(spot == j, piece, kept)
            out[q * packs + k] = jnp.where(live, kept, jnp.zeros_like(kept))
        return carry

    lax.fori_loop(0, members // packs, members_of, 0, unroll=10)


def params(mib):
    return pltpu.CompilerParams(vmem_limit_bytes=mib * MIB)


def cost(flops, bytes_accessed):
    return pl.CostEstimate(flops=flops, bytes_accessed=bytes_accessed, transcendentals=0)


def specs(*spaces):
    return [pl.BlockSpec(memory_space=space) for space in spaces]


def shards(anomaly, jacobian, foot_cols, foot_weight, obs_count, obs_weight):
    col_groups = lax.axis_size("cols")
    chans = lax.axis_size("chan")
    tile_index = lax.axis_index("cols")
    chan_index = lax.axis_index("chan")
    tile_cols, members, levels = anomaly.shape
    obs_share = jacobian.shape[0]
    block = CH // chans

    core = lax.rem(chan_index, 2)
    edge, pieces = pl.pallas_call(
        prepare_kernel,
        out_shape=(
            jax.ShapeDtypeStruct((HALO, members, levels), jnp.bfloat16),
            jax.ShapeDtypeStruct((chans, obs_share, block, levels), jnp.bfloat16),
        ),
        in_specs=specs(pl.ANY, pl.ANY),
        out_specs=tuple(specs(pl.ANY, pl.ANY)),
        scratch_shapes=[
            pltpu.VMEM((HALO, members, levels), jnp.bfloat16),
            pltpu.VMEM((chans, obs_share, block, levels), jnp.bfloat16),
            pltpu.SemaphoreType.DMA((2,)),
            pltpu.SemaphoreType.DMA((chans,)),
            pltpu.SemaphoreType.DMA((chans,)),
        ],
        compiler_params=pltpu.CompilerParams(vmem_limit_bytes=int(60.4 * MIB)),
        cost_estimate=cost(1_000_000, 3_000_000),
        name="prepare",
    )(anomaly, jacobian)
    to_side = [
        (t * chans + j, (t + (1 if j % 2 == 0 else -1)) % col_groups * chans + j)
        for t in range(col_groups)
        for j in range(chans)
    ]
    ours = lax.ppermute(edge, ("cols", "chan"), to_side)
    theirs = lax.ppermute(ours, "chan", [(j, j ^ 1) for j in range(chans)])

    jac_block = lax.all_to_all(pieces, "chan", split_axis=0, concat_axis=0, tiled=True)
    jac_block = jac_block.reshape(OBS_DEV, block, levels)

    first_obs = chan_index * obs_share
    columns = foot_cols.T
    column_gains = foot_weight.T
    offsets = jnp.mod(columns - tile_index * tile_cols + HALO, tile_cols * col_groups)
    centers = jnp.sum(column_gains * (offsets - HALO).astype(jnp.float32), axis=0) / jnp.sum(
        column_gains, axis=0
    )
    own_centers = lax.dynamic_slice_in_dim(centers, first_obs, obs_share, 0)
    spacing = tile_cols / PTS
    points = (jnp.arange(PTS, dtype=jnp.float32) + 0.5) * spacing
    locality = taper(own_centers[None, :] - points[:, None], spacing) / (CH * OBS_DEV)
    first_ours = jnp.where(core == 0, 0, HALO + tile_cols)
    low_reach = jnp.min(offsets, axis=0) < HALO
    high_reach = jnp.max(offsets, axis=0) >= HALO + tile_cols
    ours_reach = jnp.where(core == 0, low_reach, high_reach)
    theirs_reach = jnp.where(core == 0, high_reach, low_reach)
    reach = ours_reach.astype(jnp.int32) + 2 * theirs_reach.astype(jnp.int32)
    tail = jnp.stack([first_obs, first_ours]).astype(jnp.int32)
    inside = jnp.logical_and(offsets >= HALO, offsets < HALO + tile_cols)
    home_cols = jnp.clip(offsets - HALO, 0, tile_cols - 1)
    home_gains = jnp.where(inside, column_gains, 0.0)
    ints = jnp.concatenate([offsets.reshape(-1), reach, tail, home_cols.reshape(-1)])
    gains = jnp.concatenate(
        [column_gains.reshape(-1), locality.reshape(-1), home_gains.reshape(-1)]
    )

    tile = jax.ShapeDtypeStruct((OBS_DEV, members, levels), jnp.bfloat16)
    home = pl.pallas_call(
        home_kernel,
        out_shape=tile,
        in_specs=specs(SMEM, SMEM, pl.ANY),
        out_specs=pl.BlockSpec(memory_space=VMEM),
        scratch_shapes=[pltpu.VMEM(anomaly.shape, anomaly.dtype), pltpu.SemaphoreType.DMA((2,))],
        compiler_params=params(50),
        cost_estimate=cost(4_000_000_000, 8_000_000),
        name="home_mix",
    )(ints, gains, anomaly)

    gram, mixed = pl.pallas_call(
        lambda *refs: gram_kernel(tile_cols, *refs),
        out_shape=(jax.ShapeDtypeStruct((members, PTS, members), jnp.bfloat16), tile),
        in_specs=specs(SMEM, SMEM, SMEM, VMEM, VMEM, VMEM, VMEM, VMEM),
        out_specs=tuple(specs(VMEM, pl.ANY)),
        scratch_shapes=[
            pltpu.VMEM(tile.shape, tile.dtype),
            pltpu.VMEM((obs_share, members, CH), jnp.bfloat16),
            pltpu.VMEM((obs_share, members, members), jnp.float32),
            pltpu.VMEM((members * PTS, 128), jnp.float32),
            pltpu.SemaphoreType.DMA,
        ],
        compiler_params=params(46),
        cost_estimate=cost(6_000_000_000, 3_000_000),
        name="gram",
    )(obs_count, ints, gains, ours, theirs, home, jacobian, obs_weight.T)
    arrived = lax.all_to_all(gram, "chan", split_axis=0, concat_axis=0, tiled=True)
    perturbed = pl.pallas_call(
        radiance_kernel,
        out_shape=jax.ShapeDtypeStruct((members, block, OBS_DEV), jnp.bfloat16),
        in_specs=specs(SMEM, VMEM, pl.ANY),
        out_specs=pl.BlockSpec(memory_space=VMEM),
        scratch_shapes=[
            pltpu.VMEM(tile.shape, tile.dtype),
            pltpu.VMEM((members * (OBS_DEV * block // levels + 8), levels), jnp.float32),
            pltpu.SemaphoreType.DMA((2, levels // block)),
        ],
        compiler_params=params(52),
        cost_estimate=cost(4_000_000_000, 5_000_000),
        name="radiance",
    )(obs_count, jac_block, mixed)

    gram_rows = arrived.reshape(chans, members // chans, PTS, members).astype(jnp.float32).sum(0)
    return perturbed, gram_rows.transpose(1, 0, 2)


def solution(mesh):
    return jax.shard_map(
        shards,
        mesh=mesh,
        in_specs=(
            P("cols", None, None),
            P(("cols", "chan"), None, None),
            P("cols", None),
            P("cols", None),
            P("cols"),
            P(None, ("cols", "chan")),
        ),
        out_specs=(P(None, "chan", "cols"), P("cols", "chan", None)),
        check_vma=False,
    )
```

```python
import jax
import jax.numpy as jnp
from jax import lax
from jax.experimental import pallas as pl
from jax.experimental.pallas import tpu as pltpu
from jax.sharding import PartitionSpec as P


CH = 256
OBS_DEV = 128
HALO = 32
PTS = 8
FP = 4
MIB = 1024 * 1024
REACH = FP * OBS_DEV
TAIL = REACH + OBS_DEV
HOME_COLS = TAIL + 2
LOCALITY = FP * OBS_DEV
HOME_GAINS = LOCALITY + OBS_DEV
LIVE = HOME_GAINS + FP * OBS_DEV

VMEM = pltpu.MemorySpace.VMEM
SMEM = pltpu.MemorySpace.SMEM
NT = (((1,), (1,)), ((), ()))


def taper(distance, half_width):
    relative = jnp.abs(distance) / half_width
    near_part = (
        ((-0.25 * relative + 0.5) * relative + 0.625) * relative - 5.0 / 3.0
    ) * relative * relative + 1.0
    bounded = jnp.maximum(relative, 1.0)
    far_part = (
        ((((relative / 12.0 - 0.5) * relative + 0.625) * relative + 5.0 / 3.0) * relative - 5.0)
        * relative
        + 4.0
        - 2.0 / (3.0 * bounded)
    )
    return jnp.where(relative <= 1.0, near_part, jnp.where(relative <= 2.0, far_part, 0.0))


def side_mix(ints, gains, halo, n, first):
    total = None
    for f in range(FP):
        col = ints[f * OBS_DEV + n] - first
        inside = jnp.logical_and(col >= 0, col < HALO)
        gain = jnp.where(inside, gains[f * OBS_DEV + n], 0.0)
        term = gain * halo[jnp.clip(col, 0, HALO - 1)].astype(jnp.float32)
        total = term if total is None else total + term
    return total


def prepare_kernel(anomaly, jac, edge, pieces, cut, held, cut_sems, in_sems, out_sems):
    core = lax.rem(lax.axis_index("chan"), 2)
    first = jnp.where(core == 0, anomaly.shape[0] - HALO, 0)
    chans, _, block, _ = held.shape
    cut_in = pltpu.make_async_copy(anomaly.at[pl.ds(first, HALO)], cut, cut_sems.at[0])
    cut_out = pltpu.make_async_copy(cut, edge, cut_sems.at[1])
    cut_in.start()
    arrive = [
        pltpu.make_async_copy(jac.at[:, pl.ds(j * block, block)], held.at[j], in_sems.at[j])
        for j in range(chans)
    ]
    leave = [
        pltpu.make_async_copy(held.at[j], pieces.at[j], out_sems.at[j]) for j in range(chans)
    ]
    for copy in arrive:
        copy.start()
    cut_in.wait()
    cut_out.start()
    for before, after in zip(arrive, leave):
        before.wait()
        after.start()
    cut_out.wait()
    for copy in leave:
        copy.wait()


def home_kernel(ints, gains, anomaly, home, tile, sems):
    members = anomaly.shape[1]
    cuts = (0, 48, members)
    parts = [pl.ds(low, high - low) for low, high in zip(cuts, cuts[1:])]
    copies = [
        pltpu.make_async_copy(anomaly.at[:, part], tile.at[:, part], sems.at[k])
        for k, part in enumerate(parts)
    ]
    for copy in copies:
        copy.start()
    for copy, part in zip(copies, parts):
        copy.wait()

        def each(n, carry, part=part):
            total = None
            for f in range(FP):
                gain = gains[HOME_GAINS + f * OBS_DEV + n]
                term = gain * tile[ints[HOME_COLS + f * OBS_DEV + n], part].astype(jnp.float32)
                total = term if total is None else total + term
            home[n, part] = total.astype(home.dtype)
            return carry

        lax.fori_loop(0, OBS_DEV, each, 0, unroll=4)


def gram_kernel(tile_cols, ints, gains, ours, theirs, home, jac, weight, gram, mixed_out, mixed, perts, products, turned, sem):
    share, members = perts.shape[:2]
    first_obs = ints[TAIL]
    first_ours = ints[TAIL + 1]
    first_theirs = HALO + tile_cols - first_ours

    def add(n, halo, first):
        mixed[n] = (mixed[n].astype(jnp.float32) + side_mix(ints, gains, halo, n, first)).astype(
            mixed.dtype
        )

    def complete(n):
        reach = ints[REACH + n]

        @pl.when(reach > 0)
        def _():
            @pl.when(jnp.bitwise_and(reach, 1) > 0)
            def _():
                add(n, ours, first_ours)

            @pl.when(jnp.bitwise_and(reach, 2) > 0)
            def _():
                add(n, theirs, first_theirs)

    def each(q, carry):
        batch = pl.ds(q * 4, 4)
        mixed[batch] = home[batch]
        for k in range(4):
            complete(q * 4 + k)
        return carry

    lax.fori_loop(0, OBS_DEV // 4, each, 0)
    leave = pltpu.make_async_copy(mixed, mixed_out, sem)
    leave.start()
    for i in range(share):
        live = gains[LIVE + first_obs + i]
        radiance = lax.dot_general(
            mixed[first_obs + i], jac[i], NT, preferred_element_type=jnp.float32
        )
        perts[i] = (radiance * live).astype(jnp.bfloat16)
    for i in range(share):
        pert = perts[i]
        scaled = (pert.astype(jnp.float32) * weight[i : i + 1, :].astype(jnp.float32)).astype(
            jnp.bfloat16
        )
        products[i] = lax.dot_general(scaled, pert, NT, preferred_element_type=jnp.float32)
    for p in range(PTS):
        total = None
        for i in range(share):
            term = gains[LOCALITY + p * share + i] * products[i]
            total = term if total is None else total + term
        turned[pl.ds(p, members, stride=PTS), 0:members] = total
    gram[...] = turned[:, 0:members].reshape(members, PTS, members).astype(gram.dtype)
    leave.wait()


def radiance_kernel(alive, jac, mixed_ref, out, mixed, turned, sems):
    members, block, levels = mixed.shape[1], jac.shape[1], jac.shape[2]
    steps = sems.shape[0]
    packs = levels // block
    groups = OBS_DEV // packs
    pitch = groups + 8
    owner = lax.broadcasted_iota(jnp.int32, (members, levels), 1) // block

    batch = groups // steps
    copies = [
        [
            pltpu.make_async_copy(
                mixed_ref.at[pl.ds(j * groups + step * batch, batch)],
                mixed.at[pl.ds(j * groups + step * batch, batch)],
                sems.at[step, j],
            )
            for j in range(packs)
        ]
        for step in range(steps)
    ]
    for step in copies:
        for copy in step:
            copy.start()

    def group(g, carry):
        names = [g + j * groups for j in range(packs)]
        stacked = jnp.concatenate([jac[n] for n in names], axis=0)
        averages = jnp.concatenate([mixed[n] for n in names], axis=0)
        full = lax.dot_general(averages, stacked, NT, preferred_element_type=jnp.float32)
        kept = full[:members]
        for j in range(1, packs):
            kept = jnp.where(owner == j, full[j * members : (j + 1) * members], kept)
        turned[pl.ds(g, members, stride=pitch), :] = kept
        return carry

    for step in range(steps):
        for copy in copies[step]:
            copy.wait()
        lax.fori_loop(step * batch, (step + 1) * batch, group, 0, unroll=batch)
    slot = lax.broadcasted_iota(jnp.int32, (block, OBS_DEV), 1)
    spot = slot // groups
    live = jnp.broadcast_to(alive[...], slot.shape) > 0.0

    def members_of(q, carry):
        rows = [
            turned[pl.ds(pl.multiple_of((q * packs + k) * pitch, 8), groups), :].astype(out.dtype)
            for k in range(packs)
        ]
        flipped = jnp.concatenate(rows, axis=0).T
        for k in range(packs):
            kept = None
            for j in range(packs):
                piece = flipped[j * block : (j + 1) * block, :]
                shift = (j - k) * groups % OBS_DEV
                piece = piece if shift == 0 else pltpu.roll(piece, shift, 1)
                kept = piece if kept is None else jnp.where(spot == j, piece, kept)
            out[q * packs + k] = jnp.where(live, kept, jnp.zeros_like(kept))
        return carry

    lax.fori_loop(0, members // packs, members_of, 0, unroll=10)


def params(mib):
    return pltpu.CompilerParams(vmem_limit_bytes=mib * MIB)


def cost(flops, bytes_accessed):
    return pl.CostEstimate(flops=flops, bytes_accessed=bytes_accessed, transcendentals=0)


def specs(*spaces):
    return [pl.BlockSpec(memory_space=space) for space in spaces]


def shards(anomaly, jacobian, foot_cols, foot_weight, obs_count, obs_weight):
    col_groups = lax.axis_size("cols")
    chans = lax.axis_size("chan")
    tile_index = lax.axis_index("cols")
    chan_index = lax.axis_index("chan")
    tile_cols, members, levels = anomaly.shape
    obs_share = jacobian.shape[0]
    block = CH // chans

    core = lax.rem(chan_index, 2)
    edge, pieces = pl.pallas_call(
        prepare_kernel,
        out_shape=(
            jax.ShapeDtypeStruct((HALO, members, levels), jnp.bfloat16),
            jax.ShapeDtypeStruct((chans, obs_share, block, levels), jnp.bfloat16),
        ),
        in_specs=specs(pl.ANY, pl.ANY),
        out_specs=tuple(specs(pl.ANY, pl.ANY)),
        scratch_shapes=[
            pltpu.VMEM((HALO, members, levels), jnp.bfloat16),
            pltpu.VMEM((chans, obs_share, block, levels), jnp.bfloat16),
            pltpu.SemaphoreType.DMA((2,)),
            pltpu.SemaphoreType.DMA((chans,)),
            pltpu.SemaphoreType.DMA((chans,)),
        ],
        compiler_params=pltpu.CompilerParams(vmem_limit_bytes=int(60.4 * MIB)),
        cost_estimate=cost(1_000_000, 3_000_000),
        name="prepare",
    )(anomaly, jacobian)
    to_side = [
        (t * chans + j, (t + (1 if j % 2 == 0 else -1)) % col_groups * chans + j)
        for t in range(col_groups)
        for j in range(chans)
    ]
    ours = lax.ppermute(edge, ("cols", "chan"), to_side)
    theirs = lax.ppermute(ours, "chan", [(j, j ^ 1) for j in range(chans)])

    jac_block = lax.all_to_all(pieces, "chan", split_axis=0, concat_axis=0, tiled=True)
    jac_block = jac_block.reshape(OBS_DEV, block, levels)

    first_obs = chan_index * obs_share
    columns = foot_cols.T
    column_gains = foot_weight.T
    offsets = jnp.mod(columns - tile_index * tile_cols + HALO, tile_cols * col_groups)
    centers = jnp.sum(column_gains * (offsets - HALO).astype(jnp.float32), axis=0) / jnp.sum(
        column_gains, axis=0
    )
    own_centers = lax.dynamic_slice_in_dim(centers, first_obs, obs_share, 0)
    spacing = tile_cols / PTS
    points = (jnp.arange(PTS, dtype=jnp.float32) + 0.5) * spacing
    locality = taper(own_centers[None, :] - points[:, None], spacing) / (CH * OBS_DEV)
    first_ours = jnp.where(core == 0, 0, HALO + tile_cols)
    low_reach = jnp.min(offsets, axis=0) < HALO
    high_reach = jnp.max(offsets, axis=0) >= HALO + tile_cols
    ours_reach = jnp.where(core == 0, low_reach, high_reach)
    theirs_reach = jnp.where(core == 0, high_reach, low_reach)
    reach = ours_reach.astype(jnp.int32) + 2 * theirs_reach.astype(jnp.int32)
    tail = jnp.stack([first_obs, first_ours]).astype(jnp.int32)
    inside = jnp.logical_and(offsets >= HALO, offsets < HALO + tile_cols)
    home_cols = jnp.clip(offsets - HALO, 0, tile_cols - 1)
    home_gains = jnp.where(inside, column_gains, 0.0)
    ints = jnp.concatenate([offsets.reshape(-1), reach, tail, home_cols.reshape(-1)])
    alive = (jnp.arange(OBS_DEV, dtype=jnp.int32) < obs_count[0]).astype(jnp.float32)
    gains = jnp.concatenate(
        [column_gains.reshape(-1), locality.reshape(-1), home_gains.reshape(-1), alive]
    )

    tile = jax.ShapeDtypeStruct((OBS_DEV, members, levels), jnp.bfloat16)
    home = pl.pallas_call(
        home_kernel,
        out_shape=tile,
        in_specs=specs(SMEM, SMEM, pl.ANY),
        out_specs=pl.BlockSpec(memory_space=VMEM),
        scratch_shapes=[pltpu.VMEM(anomaly.shape, anomaly.dtype), pltpu.SemaphoreType.DMA((2,))],
        compiler_params=params(50),
        cost_estimate=cost(4_000_000_000, 8_000_000),
        name="home_mix",
    )(ints, gains, anomaly)

    gram, mixed = pl.pallas_call(
        lambda *refs: gram_kernel(tile_cols, *refs),
        out_shape=(jax.ShapeDtypeStruct((members, PTS, members), jnp.bfloat16), tile),
        in_specs=specs(SMEM, SMEM, VMEM, VMEM, VMEM, VMEM, VMEM),
        out_specs=tuple(specs(VMEM, pl.ANY)),
        scratch_shapes=[
            pltpu.VMEM(tile.shape, tile.dtype),
            pltpu.VMEM((obs_share, members, CH), jnp.bfloat16),
            pltpu.VMEM((obs_share, members, members), jnp.float32),
            pltpu.VMEM((members * PTS, 128), jnp.float32),
            pltpu.SemaphoreType.DMA,
        ],
        compiler_params=params(46),
        cost_estimate=cost(6_000_000_000, 3_000_000),
        name="gram",
    )(ints, gains, ours, theirs, home, jacobian, obs_weight.T)
    arrived = lax.all_to_all(gram, "chan", split_axis=0, concat_axis=0, tiled=True)
    perturbed = pl.pallas_call(
        radiance_kernel,
        out_shape=jax.ShapeDtypeStruct((members, block, OBS_DEV), jnp.bfloat16),
        in_specs=specs(VMEM, VMEM, pl.ANY),
        out_specs=pl.BlockSpec(memory_space=VMEM),
        scratch_shapes=[
            pltpu.VMEM(tile.shape, tile.dtype),
            pltpu.VMEM((members * (OBS_DEV * block // levels + 8), levels), jnp.float32),
            pltpu.SemaphoreType.DMA((2, levels // block)),
        ],
        compiler_params=params(52),
        cost_estimate=cost(4_000_000_000, 5_000_000),
        name="radiance",
    )(alive[None], jac_block, mixed)

    gram_rows = arrived.reshape(chans, members // chans, PTS, members).astype(jnp.float32).sum(0)
    return perturbed, gram_rows.transpose(1, 0, 2)


def solution(mesh):
    return jax.shard_map(
        shards,
        mesh=mesh,
        in_specs=(
            P("cols", None, None),
            P(("cols", "chan"), None, None),
            P("cols", None),
            P("cols", None),
            P("cols"),
            P(None, ("cols", "chan")),
        ),
        out_specs=(P(None, "chan", "cols"), P("cols", "chan", None)),
        check_vma=False,
    )
```
